32 devices in a mesh: src: 4 (over y, x), blk: 8 (over z, core).
Axes of the slice: x: 2, y: 2, z: 4, core: 2. Of those that a mesh axis runs over, the one named last changes fastest.
Arguments:
- values: float32 [4, 512, 32, 128], P('src', 'blk'), may hold values from -0.25 to 0.25
- diagonal: float32 [4, 512, 128], P('src', 'blk'), may hold values from 0.55 to 0.95
- rhs_parts: float32 [4, 512, 128], P('src', 'blk'), may hold values from -24 to 24
- owner_map: int32 [512, 128], P('blk'), may hold values from 0 to 3
- columns: int32 [512, 32, 128], P('blk'), may hold values from 0 to 1073741823
- destination: int32 [512, 1], P('blk'), may hold values from 0 to 7; in each aligned block of 64 rows (0 to 63, 64 to 127, ...) at most 16 rows name the same one
- order_keys: int32 [512], P('blk'), may hold values from 0 to 511, each once
Outputs:
- solution: float32 [512, 128], P('blk')
The draws below stay inside these ranges and needn't reach their ends.
Inputs may be any that keep to these rules, and one draw needn't show every extreme that they name: `destination`: among the row blocks of one index of blk no owner is named more than 16 times, some owner is named exactly 16 times, and every owner is named by some block. `order_keys`: each key appears once.
All inputs are finite; a program needn't handle non-finite values.
Results may differ from the reference program's by a relative error of at most 0.0003.
Values sent between devices are 32-bit elements; how exact they have to be, the bound alone decides.
No kernel may reach another device: no remote copies, remote signals or barrier semaphores. Data moves between devices by JAX's collectives and lax.ppermute only.
A program may use at most 64 MiB of HBM per device.

```python
import math
import jax
import jax.numpy as jnp
import numpy as np
from jax import lax

TD = 64
TR = 128
KOFF = 32
SWEEPS = 3
SEND = 16
TILES = 512
N_SRC = 4
N_BLK = 8


def with_ends(array, key, low, top_value):
    index_at = [jax.random.randint(jax.random.fold_in(key, axis), (), 0, length) for axis, length in enumerate(array.shape)]
    widest = array.shape.index(max(array.shape))
    beside = index_at[:widest] + [(index_at[widest] + 1) % array.shape[widest]] + index_at[widest + 1:]
    return array.at[tuple(index_at)].set(low).at[tuple(beside)].set(top_value)


def levels(stream_key, dims, shards, least, high):
    def one(dim, shards_of):
        heights = jax.random.uniform(jax.random.fold_in(jax.random.fold_in(stream_key, 6), dim), (shards_of,), jnp.float32, least / len(shards), high / len(shards))
        return jnp.repeat(jnp.exp(heights), dims[dim] // shards_of).reshape((-1,) + (1,) * (len(dims) - dim - 1))

    gain = one(*shards[0])
    for cut in shards[1:]:
        gain = gain * one(*cut)
    return gain


def routed_block(rng, own, number, rows, number_of, top, most, slope):
    order = jax.random.permutation(rng, number_of)
    crowded, usual = shares(number_of, rows * top, most, slope, True), shares(number_of, rows * top, most, slope, False)
    places = jnp.arange(number_of)

    def named(sizes, rotation):
        used = int((sizes > 0).sum())
        fixed = max(1, used // 4)
        moved = fixed + (places - fixed + rotation * (used - fixed)) % max(1, number_of - fixed)
        return jnp.zeros((number_of,), jnp.int32).at[order[jnp.where(places < fixed, places, moved)]].set(jnp.asarray(sizes, jnp.int32))

    sizes = jnp.where(number % 4 == 0, named(crowded, number // 4), named(usual, number - number // 4 - 1))
    mixed = jax.random.permutation(jax.random.fold_in(own, 3), number_of)
    donor, taker = mixed[0:number_of // 2 * 2:2], mixed[1:number_of // 2 * 2:2]
    room = jnp.minimum(sizes[donor] - 1, most - sizes[taker]) // 2
    room = jnp.where((donor == order[0]) | (taker == order[0]) | (sizes[taker] == 0), 0, jnp.maximum(room, 0))
    moved = jax.random.randint(jax.random.fold_in(own, 4), (number_of // 2,), 0, 1 << 20) % (room + 1)
    sizes = sizes.at[donor].add(-moved).at[taker].add(moved)
    members = jnp.searchsorted(jnp.cumsum(sizes), jnp.arange(rows * top), side="right").astype(jnp.int32)
    listing = members.reshape(top, rows).T
    listing = listing[jax.random.permutation(jax.random.fold_in(own, 1), rows)]
    rotation = jax.random.randint(jax.random.fold_in(own, 2), (rows, 1), 0, top)
    return jnp.take_along_axis(listing, (jnp.arange(top)[None, :] + rotation) % top, axis=1)


def shares(number_of, total, most, slope, full):
    loads = [(1 << 20) // math.isqrt(grade ** slope) + 1 for grade in range(1, number_of + 1)]
    largest = most if full else min(most, max(-(-total // number_of), total * loads[0] // sum(loads)))
    least = 1 if total - largest >= number_of - 1 else 0
    given, spare = [largest] + [least] * (number_of - 1), total - largest - least * (number_of - 1)
    while spare > 0:
        free = [i for i in range(1, number_of) if given[i] < largest] or [i for i in range(1, number_of) if given[i] < most]
        whole, budget = sum([loads[i] for i in free]), spare
        for i in free:
            extra = min(most - given[i], max(1, budget * loads[i] // whole), spare)
            given[i] = given[i] + extra
            spare = spare - extra
    return np.array(given)


def gaussian(rng, dims, scale, limit, shards=(), kind=jnp.bfloat16):
    loudness = levels(rng, dims, shards, -0.22, 0.18) if shards else 1.0
    result = jax.random.normal(rng, dims, jnp.float32) * scale * loudness
    return jnp.minimum(jnp.maximum(result, -limit), limit).astype(kind)


def setup_inputs(seed: int = 0) -> dict:
    splits = jax.random.split(jax.random.key(seed), 8)
    values = jnp.clip(jax.random.uniform(splits[0], (N_SRC, TILES, KOFF, TR), jnp.float32, -0.25, 0.25) * levels(splits[0], (N_SRC, TILES, KOFF, TR), ((0, 4), (1, 8)), -0.4, 0.0), -0.25, 0.25)
    diagonal = jnp.clip(0.55 + 0.39999998 * jax.random.uniform(splits[1], (N_SRC, TILES, TR), jnp.float32) ** levels(splits[1], (N_SRC, TILES, TR), ((0, 4), (1, 8)), -0.2, 0.2), 0.55, 0.95)
    rhs_parts = gaussian(splits[2], (N_SRC, TILES, TR), 4.0, 24.0, ((0, 4), (1, 8)), jnp.float32)
    owner_map = with_ends(jax.random.randint(splits[3], (TILES, TR), 0, N_SRC), jax.random.fold_in(splits[3], 1), 0, N_SRC - 1).astype(jnp.int32)
    columns = with_ends(jax.random.randint(splits[4], (TILES, KOFF, TR), 0, 1073741824), jax.random.fold_in(splits[4], 1), 0, 1073741823).astype(jnp.int32)
    destination_keys = jax.random.split(jax.random.fold_in(splits[5], 1), TILES // TD)
    destination_turns = jax.random.permutation(jax.random.fold_in(splits[5], 3), TILES // TD)
    destination = jax.vmap(lambda own, number: routed_block(jax.random.fold_in(splits[5], 2), own, number, TD, N_BLK, 1, SEND, 2))(destination_keys, destination_turns).reshape((TILES, 1))
    order_keys = jax.random.permutation(splits[6], TILES).astype(jnp.int32)
    return dict(values=values, diagonal=diagonal, rhs_parts=rhs_parts, owner_map=owner_map, columns=columns, destination=destination, order_keys=order_keys)


def reference(values, diagonal, rhs_parts, owner_map, columns, destination, order_keys):
    owner_of = destination[:, 0]
    same_owner = owner_of[:, None] == owner_of[None, :]
    tile_rank = jnp.sum(same_owner & (order_keys[None, :] < order_keys[:, None]), axis=1).astype(jnp.int32)
    owner_ids = jnp.arange(N_BLK, dtype=jnp.int32)
    owner_counts = jnp.sum(owner_of[None, :] == owner_ids[:, None], axis=1).astype(jnp.int32)
    slot_count = N_BLK * SEND
    slot_table = jnp.full((N_BLK, slot_count), -1, jnp.int32)
    slot_table = slot_table.at[owner_of, tile_rank].set(jnp.arange(TILES, dtype=jnp.int32))
    assembled = jnp.sum(values, axis=0)
    assembled_diag = jnp.sum(diagonal, axis=0)
    right_side = jnp.take_along_axis(rhs_parts, owner_map[None, :, :], axis=0)[0]
    slot_numbers = jnp.arange(slot_count, dtype=jnp.int32)

    def solve_owner(owner):
        chosen = slot_table[owner]
        is_live = chosen >= 0
        safe_index = jnp.maximum(chosen, 0)
        block_vals = jnp.where(is_live[:, None, None], assembled[safe_index], 0.0)
        block_cols = columns[safe_index]
        block_right = jnp.where(is_live[:, None], right_side[safe_index], 0.0)
        block_diag = jnp.where(is_live[:, None], assembled_diag[safe_index], 1.0)
        step_over = jnp.remainder(block_cols // TR, 2).astype(jnp.int32)
        target_tile = jnp.remainder(slot_numbers[:, None, None] + step_over, owner_counts[owner]).astype(jnp.int32)
        location = (target_tile * TR + jnp.remainder(block_cols, TR)).astype(jnp.int32)
        iterate = jnp.zeros((slot_count * TR,), jnp.float32)
        for sweep_index in range(SWEEPS):
            nearby = iterate[location]
            summed = jnp.sum(block_vals * nearby, axis=1)
            update = jnp.where(is_live[:, None], (block_right - summed) / block_diag, 0.0)
            iterate = update.reshape(-1)
        return iterate.reshape(slot_count, TR)

    solved = lax.map(solve_owner, owner_ids)
    return solved[owner_of, tile_rank]
```

```python
import jax
import jax.numpy as jnp
from jax import lax
from jax.experimental import pallas as pl
from jax.experimental.pallas import tpu as pltpu
from jax.sharding import PartitionSpec as P

SWEEPS = 3
BOTH = ("src", "blk")
HEAD = 8


def start_kernel(small_ref, owner_ref, head_ref, diag_out, right_out, send_out):
    parts = small_ref.shape[0]
    rows = diag_out.shape[0]
    owner = owner_ref[...]
    diag = small_ref[0, 0]
    right = jnp.where(owner == 0, small_ref[0, 1], 0.0)
    for part in range(1, parts):
        diag = diag + small_ref[part, 0]
        right = jnp.where(owner == part, small_ref[part, 1], right)
    diag_out[...] = diag
    right_out[...] = right
    first = right / diag
    send_out[:, :rows] = jnp.broadcast_to(first[None], (send_out.shape[0],) + first.shape)
    send_out[:, rows:] = jnp.broadcast_to(head_ref[...][None], (send_out.shape[0], HEAD, first.shape[1]))


def gather_tile(own, following, codes, rows):
    lanes = codes & (rows - 1)
    here = jnp.take_along_axis(jnp.broadcast_to(own, codes.shape), lanes, axis=1)
    there = jnp.take_along_axis(jnp.broadcast_to(following, codes.shape), lanes, axis=1)
    return jnp.where((codes & rows) == 0, here, there)


def follow(pick, everyone):
    return jnp.dot(pick, everyone, precision=lax.Precision.HIGHEST, preferred_element_type=jnp.float32)


def nearby_kernel(got_ref, own_ref, owner_ref, key_ref, codes_ref, nearby_out, pick_out, least_ref):
    tiles, _, rows = codes_ref.shape
    peers = got_ref.shape[0]
    total = peers * tiles
    owners = got_ref[:, tiles, :]
    keys = got_ref[:, tiles + 1, :]
    place = lax.broadcasted_iota(jnp.int32, owners.shape, 0) * tiles + lax.broadcasted_iota(jnp.int32, owners.shape, 1)
    place = place.astype(jnp.float32)
    for tile in range(tiles):
        ahead = keys - key_ref[tile:tile + 1, 0:1] - 1.0
        ahead = jnp.where(ahead < 0.0, ahead + total, ahead)
        code = jnp.where(owners == owner_ref[tile:tile + 1, 0:1], ahead * total + place, float(total * total))
        least_ref[tile:tile + 1] = jnp.min(code, axis=0, keepdims=True)
    chosen = jnp.min(least_ref[...], axis=1, keepdims=True).astype(jnp.int32)
    chosen = lax.rem(chosen, jnp.full_like(chosen, total))
    pick = (lax.broadcasted_iota(jnp.int32, (tiles, total), 1) == chosen).astype(jnp.float32)
    pick_out[...] = pick
    following = follow(pick, got_ref[:, :tiles, :].reshape(total, rows))
    own = own_ref[0, :tiles]
    for tile in range(tiles):
        nearby_out[tile] = gather_tile(own[tile:tile + 1], following[tile:tile + 1], codes_ref[tile], rows)


def first_sweep_kernel(*refs):
    *part_refs, nearby_ref, right_ref, diag_ref, vals_out, send_out = refs
    tiles = nearby_ref.shape[0]
    sums = []
    for tile in range(tiles):
        vals = part_refs[0][tile]
        for part in part_refs[1:]:
            vals = vals + part[tile]
        vals_out[tile] = vals
        sums.append(jnp.sum(vals * nearby_ref[tile], axis=0, keepdims=True))
    iterate = (right_ref[...] - jnp.concatenate(sums, axis=0)) / diag_ref[...]
    send_out[...] = jnp.broadcast_to(iterate[None], send_out.shape)


def sweep_kernel(got_ref, own_ref, pick_ref, codes_ref, vals_ref, right_ref, diag_ref, send_out):
    tiles, _, rows = codes_ref.shape
    following = follow(pick_ref[...], got_ref[...].reshape(-1, rows))
    own = own_ref[0]
    sums = []
    for tile in range(tiles):
        nearby = gather_tile(own[tile:tile + 1], following[tile:tile + 1], codes_ref[tile], rows)
        sums.append(jnp.sum(vals_ref[tile] * nearby, axis=0, keepdims=True))
    iterate = (right_ref[...] - jnp.concatenate(sums, axis=0)) / diag_ref[...]
    send_out[...] = jnp.broadcast_to(iterate[None], send_out.shape)


def call(kernel, shapes, *args, scratch=()):
    vmem = pl.BlockSpec(memory_space=pltpu.VMEM)
    shapes = [jax.ShapeDtypeStruct(shape, jnp.float32) for shape in shapes]
    return pl.pallas_call(
        kernel, out_shape=shapes, in_specs=[vmem] * len(args), out_specs=[vmem] * len(shapes), scratch_shapes=scratch
    )(*args)


def on_device(values, diagonal, rhs_parts, owner_map, columns, destination, order_keys):
    parts = lax.axis_size("src")
    me = lax.axis_index("src")
    peers = parts * lax.axis_size("blk")
    held, stored, rows = values.shape[1:]
    mine = held // parts
    vec = (mine, rows)
    mat = (mine, stored, rows)

    def cut(array, part):
        return lax.dynamic_slice_in_dim(array, part * mine, mine, 0)

    small = jnp.stack([diagonal[0].reshape((parts,) + vec), rhs_parts[0].reshape((parts,) + vec)], axis=1)
    got_small = lax.all_to_all(small, "src", 0, 0, tiled=True)
    pieces = [cut(values[0], me)]
    for step in range(1, parts):
        piece = cut(values[0], jnp.remainder(me + step, parts))
        pieces.append(lax.ppermute(piece, "src", [(i, (i + step) % parts) for i in range(parts)]))
    own_map = cut(owner_map, me)
    codes = cut(columns, me)
    own_owner = cut(destination, me).astype(jnp.float32)
    own_key = cut(order_keys[:, None], me).astype(jnp.float32)
    head = jnp.concatenate([own_owner.T, own_key.T], axis=0)
    head = jnp.pad(head, ((0, HEAD - 2), (0, rows - mine)), constant_values=-1.0)

    diag, right, send = call(start_kernel, [vec, vec, (peers, mine + HEAD, rows)], got_small, own_map, head)
    got = lax.all_to_all(send, BOTH, 0, 0, tiled=True)
    nearby, pick = call(
        nearby_kernel, [mat, (mine, mine * peers)], got, send, own_owner, own_key, codes,
        scratch=[pltpu.VMEM(vec, jnp.float32)],
    )
    vals, send = call(first_sweep_kernel, [mat, (peers,) + vec], *pieces, nearby, right, diag)
    for sweep in range(2, SWEEPS):
        last = sweep == SWEEPS - 1
        got = lax.all_to_all(send, BOTH, 0, 0, tiled=True)
        (send,) = call(sweep_kernel, [((1 if last else peers),) + vec], got, send, pick, codes, vals, right, diag)
    return lax.all_gather(send[0], "src", axis=0, tiled=True)


def solution(mesh):
    placed = (
        P("src", "blk", None, None),
        P("src", "blk", None),
        P("src", "blk", None),
        P("blk", None),
        P("blk", None, None),
        P("blk", None),
        P("blk"),
    )
    return jax.shard_map(
        on_device, mesh=mesh, in_specs=placed, out_specs=P("blk", None), check_vma=False
    )
```
